256 devices in a mesh: units: 64 (over x, z, core), expert: 4 (over y).
Axes of the slice: x: 4, y: 4, z: 8, core: 2. Of those that a mesh axis runs over, the one named last changes fastest.
Arguments:
- a_up: float32 [57344, 2048], P(('expert', 'units')), parts along dimension 0, may hold values from -6 to 6
- a_down: float32 [57344, 2048], P(('expert', 'units')), parts along dimension 0, may hold values from -6 to 6
- b_up: float32 [57344, 2048], P(('expert', 'units')), parts along dimension 0, may hold values from -6 to 6
- b_down: float32 [57344, 2048], P(('expert', 'units')), parts along dimension 0, may hold values from -6 to 6
- perm: int32 [57344], P('expert'), parts along dimension 0, may hold values from 0 to 14335, as said below
Outputs:
- merged_up: float32 [57344, 2048], P(('expert', 'units')), parts along dimension 0
- merged_down: float32 [57344, 2048], P(('expert', 'units')), parts along dimension 0
The draws below stay inside these ranges and needn't reach their ends.
There are 4 independent parts, one for each index of `expert`. The reference program is written for one: setup_inputs(seed, part) draws one part's arguments, and reference() takes and returns one part's arrays. A program takes and returns all parts, laid end to end along the dimension named above; each array names one. Nothing has to cross between parts.
Inputs may be any that keep to these rules, and one draw needn't show every extreme that they name: perm names each of the 14336 units once. Cut the units into aligned blocks of 224: of the units of one source block, at most 5 are matched to units of any one destination block, and in every draw some pair of blocks reaches 5. Every source block sends the same list of counts to the destination blocks, in an order that differs from source to source.
All inputs are finite; a program needn't handle non-finite values.
Results may differ from the reference program's by a relative error of at most 0.00002.
Values sent between devices are 32-bit elements; how exact they have to be, the bound alone decides.
No kernel may reach another device: no remote copies, remote signals or barrier semaphores. Data moves between devices by JAX's collectives and lax.ppermute only.
A program may use at most 64 MiB of HBM per device.

```python
import jax
import jax.numpy as jnp

FF = 14336
DW = 2048
CAP = 5
N_UNITS = 64


def draw_perm(key, part):
    per_dev = FF // N_UNITS
    count = N_UNITS
    limit = CAP
    keys = jax.random.split(jax.random.fold_in(key, 7), 6)
    spans = jax.random.randint(keys[0], (count,), limit - 1, limit + 1).astype(jnp.int32)
    spans = spans.at[0].set(limit)
    taken = jnp.cumsum(spans) - spans
    pieces = jnp.clip(per_dev - taken, 0, spans).astype(jnp.int32)
    ends = jnp.cumsum(pieces)
    slot = jnp.arange(per_dev, dtype=jnp.int32)
    which = jnp.sum((slot[:, None] >= ends[None, :]).astype(jnp.int32), axis=1)
    sigma = jax.random.permutation(keys[1], count).astype(jnp.int32)
    tau = jax.random.permutation(keys[2], count).astype(jnp.int32)
    sigma_inv = jnp.argsort(sigma).astype(jnp.int32)
    tau_inv = jnp.argsort(tau).astype(jnp.int32)
    source_order = jax.vmap(lambda subkey: jax.random.permutation(subkey, per_dev))(jax.random.split(keys[3], count)).astype(jnp.int32)
    target_order = jax.vmap(lambda subkey: jax.random.permutation(subkey, per_dev))(jax.random.split(keys[4], count)).astype(jnp.int32)
    dest = jnp.arange(count, dtype=jnp.int32)[:, None]
    source = tau_inv[(sigma_inv[dest] - which[None, :]) % count]
    dest_rows = dest * per_dev + target_order
    source_rows = source * per_dev + source_order[source, slot[None, :]]
    result = jnp.zeros((count * per_dev,), jnp.int32).at[dest_rows.reshape(-1)].set(source_rows.reshape(-1))
    return result


def shard_levels(key, shape, cuts, smallest, high):
    level = 1.0
    for axis_at, shards_of in cuts:
        steps = jax.random.uniform(jax.random.fold_in(jax.random.fold_in(key, 6), axis_at), (shards_of,), jnp.float32, smallest / len(cuts), high / len(cuts))
        level = level * jnp.repeat(jnp.exp(steps), shape[axis_at] // shards_of).reshape((-1,) + (1,) * (len(shape) - 1 - axis_at))
    return level


def bell_draw(stream_key, extent, deviation, reach, cuts=(), kind=jnp.bfloat16):
    array = jax.random.normal(stream_key, extent, jnp.float32) * deviation
    if len(cuts) > 0:
        array = shard_levels(stream_key, extent, cuts, -0.22, 0.18) * array
    return jnp.clip(array, min=-reach, max=reach).astype(kind)


def setup_inputs(seed: int = 0, part: int = 0) -> dict:
    key_of = jax.random.split(jax.random.key(seed), 6)
    own_keys = jax.random.split(jax.random.fold_in(key_of[5], part), 6)
    a_up = bell_draw(own_keys[0], (FF, DW), 1.0, 6.0, ((0, 64),), jnp.float32)
    a_down = bell_draw(own_keys[1], (FF, DW), 1.0, 6.0, ((0, 64),), jnp.float32)
    b_up = bell_draw(own_keys[2], (FF, DW), 1.0, 6.0, ((0, 64),), jnp.float32)
    b_down = bell_draw(own_keys[3], (FF, DW), 1.0, 6.0, ((0, 64),), jnp.float32)
    perm = draw_perm(jax.random.fold_in(jax.random.fold_in(key_of[5], part), 71), part)
    return {"a_up": a_up, "a_down": a_down, "b_up": b_up, "b_down": b_down, "perm": perm}


def reference(a_up, a_down, b_up, b_down, perm):
    permuted_up = jnp.take(b_up, perm, axis=0)
    permuted_down = jnp.take(b_down, perm, axis=0)
    merged_up = (a_up + permuted_up) * 0.5
    merged_down = (a_down + permuted_down) * 0.5
    return merged_up, merged_down
```

```python
import functools

import jax
import jax.numpy as jnp
from jax import lax
from jax.experimental import pallas as pl
from jax.experimental.pallas import tpu as pltpu
from jax.sharding import Mesh
from jax.sharding import PartitionSpec as P

UNITS = ("units_0", "units_1", "units_2")
EXCHANGE = ("units_1", "units_2", "units_0")
EXPERT_UNITS = ("expert", "units_0", "units_1", "units_2")
NX, NZ, NC = 4, 8, 2
COUNT = NX * NZ * NC
ROWS = 224
LIMIT = 5
WIDTH = 2048
TALL = WIDTH // 128
BIG = 1 << 24


def unit_of(place):
    return (place % NX) * (NZ * NC) + (place // (NX * NC)) * NC + (place // NX) % NC


def smallest(keys):
    found = []
    for _ in range(LIMIT):
        low = jnp.min(keys, axis=0, keepdims=True)
        found.append(low)
        keys = jnp.where(keys == low, BIG, keys)
    return found


def tables(perm_ref, table_ref):
    me = lax.axis_index(UNITS)
    perm = perm_ref[...]
    unit = lax.broadcasted_iota(jnp.int32, (ROWS, COUNT), 1)
    row = lax.broadcasted_iota(jnp.int32, (ROWS, COUNT), 0)
    local = perm - me * ROWS
    sends = smallest(jnp.where((local >= 0) & (local < ROWS), local, BIG))
    mine = jnp.sum(jnp.where(unit == me, perm, 0), axis=1, keepdims=True)
    local = mine - unit * ROWS
    takes = smallest(jnp.where((local >= 0) & (local < ROWS), local * 256 + row, BIG))
    for r in range(LIMIT):
        table_ref[r : r + 1, 0:COUNT] = jnp.where(sends[r] >= BIG, 0, sends[r])
        table_ref[8 + r : 9 + r, 0:COUNT] = jnp.where(takes[r] >= BIG, ROWS, takes[r] & 255)


def pack_kernel(perm_ref, up_ref, down_ref, send_ref, takes_ref, up, down, table, scalars, sems):
    loads = [
        pltpu.make_async_copy(up_ref, up, sems.at[0]),
        pltpu.make_async_copy(down_ref, down, sems.at[1]),
    ]
    for load in loads:
        load.start()
    tables(perm_ref, table)
    takes_ref[...] = table[8:16, :]
    out = pltpu.make_async_copy(table.at[0:8], scalars, sems.at[2])
    out.start()
    out.wait()
    for load in loads:
        load.wait()

    def fill(place, carry):
        unit = unit_of(place)
        for r in range(LIMIT):
            i = scalars[r, unit]
            start = (i // 8) * (8 * TALL) + i % 8
            at = pl.multiple_of((place * LIMIT + r) * (2 * TALL), 2 * TALL)
            send_ref[pl.ds(at, TALL), :] = up[pl.ds(start, TALL, stride=8), :]
            send_ref[pl.ds(at + TALL, TALL), :] = down[pl.ds(start, TALL, stride=8), :]
        return carry

    lax.fori_loop(0, COUNT, fill, 0)


def unpack_kernel(takes_ref, recv_ref, up_ref, down_ref, out_up, out_down, up, down):
    def place_rows(place, carry):
        unit = unit_of(place)
        for r in range(LIMIT):
            i = takes_ref[r, unit]
            start = (i // 8) * (8 * TALL) + i % 8
            at = pl.multiple_of((place * LIMIT + r) * (2 * TALL), 2 * TALL)
            up[pl.ds(start, TALL, stride=8), :] = recv_ref[pl.ds(at, TALL), :]
            down[pl.ds(start, TALL, stride=8), :] = recv_ref[pl.ds(at + TALL, TALL), :]
        return carry

    lax.fori_loop(0, COUNT, place_rows, 0)
    flat = ROWS * TALL
    out_up[...] = (up_ref[...] + up[0:flat, :]) * 0.5
    out_down[...] = (down_ref[...] + down[0:flat, :]) * 0.5


def tiles_of(x):
    return x.reshape(ROWS // 8, 8, TALL, 128).transpose(0, 2, 1, 3).reshape(ROWS * TALL, 128)


def rows_of(x):
    return x.reshape(ROWS // 8, TALL, 8, 128).transpose(0, 2, 1, 3).reshape(ROWS, WIDTH)


def on_device(a_up, a_down, b_up, b_down, perm):
    flat = ROWS * TALL
    slots = COUNT * LIMIT * 2 * TALL
    vmem = pl.BlockSpec(memory_space=pltpu.VMEM)
    smem = pl.BlockSpec(memory_space=pltpu.SMEM)
    hbm = pl.BlockSpec(memory_space=pl.ANY)
    send, takes = pl.pallas_call(
        pack_kernel,
        name="pack",
        out_shape=(
            jax.ShapeDtypeStruct((slots, 128), jnp.float32),
            jax.ShapeDtypeStruct((8, 128), jnp.int32),
        ),
        in_specs=[vmem, hbm, hbm],
        out_specs=(vmem, vmem),
        scratch_shapes=[
            pltpu.VMEM((flat, 128), jnp.float32),
            pltpu.VMEM((flat, 128), jnp.float32),
            pltpu.VMEM((16, 128), jnp.int32),
            pltpu.SMEM((8, 128), jnp.int32),
            pltpu.SemaphoreType.DMA((3,)),
        ],
    )(perm.reshape(COUNT, ROWS).T, tiles_of(b_up), tiles_of(b_down))
    recv = lax.all_to_all(
        send.reshape(COUNT, LIMIT * 2 * TALL, 128), EXCHANGE, split_axis=0, concat_axis=0, tiled=True
    ).reshape(slots, 128)
    merged_up, merged_down = pl.pallas_call(
        unpack_kernel,
        name="unpack",
        out_shape=(
            jax.ShapeDtypeStruct((flat, 128), jnp.float32),
            jax.ShapeDtypeStruct((flat, 128), jnp.float32),
        ),
        in_specs=[smem, vmem, vmem, vmem],
        out_specs=(vmem, vmem),
        scratch_shapes=[
            pltpu.VMEM((flat + 8 * TALL, 128), jnp.float32),
            pltpu.VMEM((flat + 8 * TALL, 128), jnp.float32),
        ],
    )(takes, recv, tiles_of(a_up), tiles_of(a_down))
    return rows_of(merged_up), rows_of(merged_down)


def solution(mesh):
    finer = Mesh(
        mesh.devices.reshape(NX, NZ, NC, mesh.shape["expert"]),
        ("units_0", "units_1", "units_2", "expert"),
    )
    rows = P(EXPERT_UNITS, None)
    return jax.shard_map(
        on_device,
        mesh=finer,
        in_specs=(rows, rows, rows, rows, P("expert")),
        out_specs=(rows, rows),
        check_vma=False,
    )
```

```python
import functools

import jax
import jax.numpy as jnp
from jax import lax
from jax.experimental import pallas as pl
from jax.experimental.pallas import tpu as pltpu
from jax.sharding import Mesh
from jax.sharding import PartitionSpec as P

UNITS = ("units_0", "units_1", "units_2")
EXCHANGE = ("units_1", "units_2", "units_0")
EXPERT_UNITS = ("expert", "units_0", "units_1", "units_2")
NX, NZ, NC = 4, 8, 2
COUNT = NX * NZ * NC
ROWS = 224
LIMIT = 5
WIDTH = 2048
TALL = WIDTH // 128
BIG = 1 << 24


def unit_of(x, z, c):
    return x * (NZ * NC) + z * NC + c


def place_of(x, z, c):
    return (z * NC + c) * NX + x


def owner(local):
    return jnp.floor((local.astype(jnp.float32) + 0.5) * (1.0 / ROWS)).astype(jnp.int32)


def send_table(perm, me, table_ref):
    local = perm - me * ROWS
    keys = jnp.where((local >= 0) & (local < ROWS), local, BIG)
    for r in range(LIMIT):
        low = jnp.min(keys, axis=0, keepdims=True)
        table_ref[r : r + 1, 0:COUNT] = jnp.where(low >= BIG, 0, low)
        keys = jnp.where(keys == low, BIG, keys)


def take_table(perm, perm_row, me):
    unit = lax.broadcasted_iota(jnp.int32, (ROWS, COUNT), 1)
    column = jnp.sum(jnp.where(unit == me, perm, 0), axis=1, keepdims=True)
    source = owner(perm_row)
    before = (owner(column) == source) & (column < perm_row)
    rank = jnp.sum(jnp.where(before, 1, 0), axis=0, keepdims=True)
    return place_of(source >> 4, (source >> 1) & 7, source & 1) * LIMIT + rank


def tables_kernel(perm_ref, blocks_ref, sends_ref, takes_ref):
    me = lax.axis_index(UNITS)
    send_table(perm_ref[...], me, sends_ref)
    takes_ref[0:1, 0:ROWS] = take_table(perm_ref[...], blocks_ref[pl.ds(me, 1), :], me)


def pack_kernel(sends_ref, up_ref, down_ref, send_ref):
    def fill(z, carry):
        for c in range(NC):
            for x in range(NX):
                for r in range(LIMIT):
                    i = sends_ref[r, unit_of(x, z, c)]
                    where = pl.ds((i >> 3) * (8 * TALL) + (i & 7), TALL, stride=8)
                    at = pl.multiple_of((place_of(x, z, c) * LIMIT + r) * (2 * TALL), 2 * TALL)
                    send_ref[pl.ds(at, TALL), :] = up_ref[where, :]
                    send_ref[pl.ds(at + TALL, TALL), :] = down_ref[where, :]
        return carry

    lax.fori_loop(0, NZ, fill, 0)


def unpack_kernel(takes_ref, recv_ref, up_ref, down_ref, out_up, out_down, up, down, sems):
    steps = 7
    part = ROWS // steps

    def stores(step):
        rows = pl.ds(step * (part * TALL), part * TALL)
        return (
            pltpu.make_async_copy(up.at[rows], out_up.at[rows], sems.at[0, step]),
            pltpu.make_async_copy(down.at[rows], out_down.at[rows], sems.at[1, step]),
        )

    for step in range(steps):

        def merge(group, carry):
            for r in range(8):
                at = pl.multiple_of(takes_ref[0, group * 8 + r] * (2 * TALL), 2 * TALL)
                where = pl.ds(group * (8 * TALL) + r, TALL, stride=8)
                up[where, :] = (up_ref[where, :] + recv_ref[pl.ds(at, TALL), :]) * 0.5
                down[where, :] = (down_ref[where, :] + recv_ref[pl.ds(at + TALL, TALL), :]) * 0.5
            return carry

        lax.fori_loop(step * (part // 8), (step + 1) * (part // 8), merge, 0)
        for store in stores(step):
            store.start()
    for step in range(steps):
        for store in stores(step):
            store.wait()


def tiles_of(x):
    return x.reshape(ROWS // 8, 8, TALL, 128).transpose(0, 2, 1, 3).reshape(ROWS * TALL, 128)


def rows_of(x):
    return x.reshape(ROWS // 8, TALL, 8, 128).transpose(0, 2, 1, 3).reshape(ROWS, WIDTH)


def on_device(a_up, a_down, b_up, b_down, perm):
    flat = ROWS * TALL
    slots = COUNT * LIMIT * 2 * TALL
    vmem = pl.BlockSpec(memory_space=pltpu.VMEM)
    smem = pl.BlockSpec(memory_space=pltpu.SMEM)
    hbm = pl.BlockSpec(memory_space=pltpu.HBM)
    blocks = perm.reshape(COUNT, ROWS)
    sends, takes = pl.pallas_call(
        tables_kernel,
        name="tables",
        out_shape=(jax.ShapeDtypeStruct((8, 128), jnp.int32), jax.ShapeDtypeStruct((8, 256), jnp.int32)),
        in_specs=[vmem, vmem],
        out_specs=(vmem, vmem),
        cost_estimate=pl.CostEstimate(flops=2_000_000_000, bytes_accessed=1 << 20, transcendentals=0),
        compiler_params=pltpu.CompilerParams(vmem_limit_bytes=4 << 20),
    )(blocks.T, blocks)
    send = pl.pallas_call(
        pack_kernel,
        name="pack",
        out_shape=jax.ShapeDtypeStruct((slots, 128), jnp.float32),
        in_specs=[smem, vmem, vmem],
        out_specs=vmem,
        compiler_params=pltpu.CompilerParams(vmem_limit_bytes=12 << 20),
    )(sends, tiles_of(b_up), tiles_of(b_down))
    recv = lax.all_to_all(
        send.reshape(COUNT, LIMIT * 2 * TALL, 128), EXCHANGE, split_axis=0, concat_axis=0, tiled=True
    ).reshape(slots, 128)
    merged_up, merged_down = pl.pallas_call(
        unpack_kernel,
        name="unpack",
        out_shape=(
            jax.ShapeDtypeStruct((flat, 128), jnp.float32),
            jax.ShapeDtypeStruct((flat, 128), jnp.float32),
        ),
        in_specs=[smem, vmem, vmem, vmem],
        out_specs=(hbm, hbm),
        scratch_shapes=[
            pltpu.VMEM((flat, 128), jnp.float32),
            pltpu.VMEM((flat, 128), jnp.float32),
            pltpu.SemaphoreType.DMA((2, 7)),
        ],
        compiler_params=pltpu.CompilerParams(vmem_limit_bytes=20 << 20),
    )(takes, recv, tiles_of(a_up), tiles_of(a_down))
    return rows_of(merged_up), rows_of(merged_down)


def solution(mesh):
    finer = Mesh(
        mesh.devices.reshape(NX, NZ, NC, mesh.shape["expert"]),
        ("units_0", "units_1", "units_2", "expert"),
    )
    rows = P(EXPERT_UNITS, None)
    return jax.shard_map(
        on_device,
        mesh=finer,
        in_specs=(rows, rows, rows, rows, P("expert")),
        out_specs=(rows, rows),
        check_vma=False,
    )
```

```python
import functools

import jax
import jax.numpy as jnp
from jax import lax
from jax.experimental import pallas as pl
from jax.experimental.pallas import tpu as pltpu
from jax.sharding import Mesh
from jax.sharding import PartitionSpec as P

UNITS = ("units_0", "units_1", "units_2")
EXPERT_UNITS = ("expert", "units_0", "units_1", "units_2")
NX, NZ, NC = 4, 8, 2
COUNT = NX * NZ * NC
LINES = NX * NC
ROWS = 224
LIMIT = 5
WIDTH = 2048
TALL = WIDTH // 128
FLAT = ROWS * TALL
CELL = LIMIT * TALL
BLOCK = LINES * CELL
BIG = 1 << 24
Z_ORDER = (4, 3, 5, 2, 6, 1, 7)
LINE_ORDER = (4, 2, 6, 5, 3, 7, 1)


def unit_at(line, dz, sign):
    x = (lax.axis_index("units_0") + sign * (line >> 1)) & (NX - 1)
    z = (lax.axis_index("units_1") + sign * dz) & (NZ - 1)
    c = (lax.axis_index("units_2") + sign * (line & 1)) & (NC - 1)
    return (x * NZ + z) * NC + c


def extract(keys):
    for r in range(LIMIT):
        low = jnp.min(keys, axis=0, keepdims=True)
        yield r, low
        keys = jnp.where(keys == low, BIG, keys)


def tables_kernel(perm_ref, sends_ref, takes_ref):
    me = lax.axis_index(UNITS)
    perm = perm_ref[...]
    unit = lax.broadcasted_iota(jnp.int32, (ROWS, COUNT), 1)
    row = lax.broadcasted_iota(jnp.int32, (ROWS, COUNT), 0)
    local = perm - me * ROWS
    for r, low in extract(jnp.where((local >= 0) & (local < ROWS), local, BIG)):
        sends_ref[r : r + 1, 0:COUNT] = jnp.where(low >= BIG, 0, low)
    mine = jnp.sum(jnp.where(unit == me, perm, 0), axis=1, keepdims=True)
    local = mine - unit * ROWS
    for r, low in extract(jnp.where((local >= 0) & (local < ROWS), local * 256 + row, BIG)):
        takes_ref[r : r + 1, 0:COUNT] = jnp.where(low >= BIG, ROWS, low & 255)


def row_at(i):
    return pl.ds((i >> 3) * (8 * TALL) + (i & 7), TALL, stride=8)


def cell(at, r):
    return pl.ds(pl.multiple_of(at * CELL + r * TALL, TALL), TALL)


def pack_by_z_kernel(sends_ref, rows_ref, *blocks):
    for dz, block in enumerate(blocks):

        def fill(line, carry):
            unit = unit_at(line, dz, 1)
            for r in range(LIMIT):
                block[cell(line, r), :] = rows_ref[row_at(sends_ref[r, unit]), :]
            return carry

        lax.fori_loop(0, LINES, fill, 0)


def pack_by_line_kernel(sends_ref, rows_ref, *blocks):
    for line, block in enumerate(blocks):

        def fill(dz, carry):
            unit = unit_at(line, dz, 1)
            for r in range(LIMIT):
                block[cell(dz, r), :] = rows_ref[row_at(sends_ref[r, unit]), :]
            return carry

        lax.fori_loop(0, NZ, fill, 0)


def turn_kernel(*refs):
    sources, targets = refs[:8], refs[8:]
    for i in range(8):
        for j in range(8):
            targets[j][i * CELL : (i + 1) * CELL, :] = sources[i][j * CELL : (j + 1) * CELL, :]


def merge(takes_ref, own_ref, block, merged, unit_of):
    def place(at, carry):
        unit = unit_of(at)
        for r in range(LIMIT):
            i = takes_ref[r, unit]
            own = own_ref[row_at(jnp.minimum(i, ROWS - 1)), :]
            merged[row_at(i), :] = (own + block[cell(at, r), :]) * 0.5
        return carry

    lax.fori_loop(0, 8, place, 0)


def store(merged, out_ref, sem):
    copy = pltpu.make_async_copy(merged.at[0:FLAT], out_ref, sem)
    copy.start()
    copy.wait()


def unpack_by_line_kernel(takes_ref, own_ref, *refs):
    blocks, (out_ref, merged, sem) = refs[:LINES], refs[LINES:]
    for line, block in enumerate(blocks):
        merge(takes_ref, own_ref, block, merged, lambda dz: unit_at(line, dz, -1))
    store(merged, out_ref, sem)


def unpack_early_kernel(shifts, takes_ref, own_ref, *refs):
    blocks, merged = refs[:-1], refs[-1]
    for dz, block in zip(shifts, blocks):
        merge(takes_ref, own_ref, block, merged, lambda line: unit_at(line, dz, -1))


def unpack_late_kernel(shifts, takes_ref, own_ref, early_ref, *refs):
    blocks, (out_ref, merged, sem) = refs[: len(shifts)], refs[len(shifts) :]
    merged[...] = early_ref[...]
    for dz, block in zip(shifts, blocks):
        merge(takes_ref, own_ref, block, merged, lambda line: unit_at(line, dz, -1))
    store(merged, out_ref, sem)


def tiles_of(x):
    return x.reshape(ROWS // 8, 8, TALL, 128).transpose(0, 2, 1, 3).reshape(FLAT, 128)


def rows_of(x):
    return x.reshape(ROWS // 8, TALL, 8, 128).transpose(0, 2, 1, 3).reshape(ROWS, WIDTH)


def sent(block, dx, dz, dc):
    def at(x, z, c):
        return (x % NX * NZ + z % NZ) * NC + c % NC

    pairs = [
        (at(x, z, c), at(x + dx, z + dz, c + dc)) for x in range(NX) for z in range(NZ) for c in range(NC)
    ]
    return lax.ppermute(block, UNITS, pairs)


def by_z(blocks):
    blocks = list(blocks)
    for dz in Z_ORDER:
        blocks[dz] = sent(blocks[dz], 0, dz, 0)
    return blocks


def by_line(blocks):
    blocks = list(blocks)
    for line in LINE_ORDER:
        blocks[line] = sent(blocks[line], line >> 1, 0, line & 1)
    return blocks


VMEM = pl.BlockSpec(memory_space=pltpu.VMEM)
SMEM = pl.BlockSpec(memory_space=pltpu.SMEM)
HBM = pl.BlockSpec(memory_space=pltpu.HBM)
PACKED = (jax.ShapeDtypeStruct((BLOCK, 128), jnp.float32),) * 8
MERGED = (FLAT + 8 * TALL, 128)
SCRATCH = [pltpu.VMEM(MERGED, jnp.float32), pltpu.SemaphoreType.DMA]


def call(kernel, name, out, specs, out_specs, scratch=(), flops=500_000_000):
    return pl.pallas_call(
        kernel,
        name=name,
        out_shape=out,
        in_specs=specs,
        out_specs=out_specs,
        scratch_shapes=list(scratch),
        cost_estimate=pl.CostEstimate(flops=flops, bytes_accessed=1 << 20, transcendentals=0),
        compiler_params=pltpu.CompilerParams(vmem_limit_bytes=12 << 20),
    )


def on_device(a_up, a_down, b_up, b_down, perm):
    out = jax.ShapeDtypeStruct((FLAT, 128), jnp.float32)
    table = jax.ShapeDtypeStruct((8, 128), jnp.int32)
    sends, takes = call(tables_kernel, "tables", (table, table), [VMEM], (VMEM, VMEM), flops=2_000_000_000)(
        perm.reshape(COUNT, ROWS).T
    )
    pack_specs = ([SMEM, VMEM], (VMEM,) * 8)
    turn_specs = ([VMEM] * 8, (VMEM,) * 8)
    down = call(pack_by_z_kernel, "pack_down", PACKED, *pack_specs)(sends, tiles_of(b_down))
    down = by_z(down)
    up = call(pack_by_line_kernel, "pack_up", PACKED, *pack_specs)(sends, tiles_of(b_up))
    up = by_line(up)
    up = call(turn_kernel, "turn_up", PACKED, *turn_specs)(*up)
    up = by_z(up)
    down = call(turn_kernel, "turn_down", PACKED, *turn_specs)(*down)
    down = by_line(down)
    merged_down = call(
        unpack_by_line_kernel, "unpack_down", out, [SMEM, VMEM] + [VMEM] * LINES, HBM, SCRATCH
    )(takes, tiles_of(a_down), *down)
    late = Z_ORDER[-2:]
    early = (0,) + Z_ORDER[:-2]
    own = tiles_of(a_up)
    merged_up = call(
        functools.partial(unpack_early_kernel, early),
        "unpack_early",
        jax.ShapeDtypeStruct(MERGED, jnp.float32),
        [SMEM, VMEM] + [VMEM] * len(early),
        VMEM,
    )(takes, own, *[up[dz] for dz in early])
    merged_up = call(
        functools.partial(unpack_late_kernel, late),
        "unpack_late",
        out,
        [SMEM, VMEM, VMEM] + [VMEM] * len(late),
        HBM,
        SCRATCH,
    )(takes, own, merged_up, *[up[dz] for dz in late])
    return rows_of(merged_up), rows_of(merged_down)


def solution(mesh):
    finer = Mesh(
        mesh.devices.reshape(NX, NZ, NC, mesh.shape["expert"]),
        ("units_0", "units_1", "units_2", "expert"),
    )
    rows = P(EXPERT_UNITS, None)
    return jax.shard_map(
        on_device,
        mesh=finer,
        in_specs=(rows, rows, rows, rows, P("expert")),
        out_specs=(rows, rows),
        check_vma=False,
    )
```

```python
import functools

import jax
import jax.numpy as jnp
from jax import lax
from jax.experimental import pallas as pl
from jax.experimental.pallas import tpu as pltpu
from jax.sharding import Mesh
from jax.sharding import PartitionSpec as P


UNITS = ("units_0", "units_1", "units_2")
EXPERT_UNITS = ("expert", "units_0", "units_1", "units_2")
NX, NZ, NC = 4, 8, 2
COUNT = NX * NZ * NC
LINES = NX * NC
ROWS = 224
LIMIT = 5
WIDTH = 2048
TALL = WIDTH // 128
FLAT = ROWS * TALL
CELL = LIMIT * TALL
BLOCK = LINES * CELL
BIG = 1 << 24
Z_ORDER = (1, 7, 2, 6, 3, 5, 4)
LINE_ORDER = (4, 2, 6, 5, 3, 7, 1)


def unit_at(line, dz, sign):
    x = (lax.axis_index("units_0") + sign * (line >> 1)) & (NX - 1)
    z = (lax.axis_index("units_1") + sign * dz) & (NZ - 1)
    c = (lax.axis_index("units_2") + sign * (line & 1)) & (NC - 1)
    return (x * NZ + z) * NC + c


def offset(row):
    return (row >> 3) * (8 * TALL) + (row & 7)


def extract(keys):
    for r in range(LIMIT):
        low = jnp.min(keys, axis=0, keepdims=True)
        yield r, low
        keys = jnp.where(keys == low, BIG, keys)


def tables_kernel(perm_ref, sends_ref, takes_ref):
    me = lax.axis_index(UNITS)
    perm = perm_ref[...]
    unit = lax.broadcasted_iota(jnp.int32, (ROWS, COUNT), 1)
    row = lax.broadcasted_iota(jnp.int32, (ROWS, COUNT), 0)
    local = perm - me * ROWS
    for r, low in extract(jnp.where((local >= 0) & (local < ROWS), local, BIG)):
        sends_ref[r : r + 1, 0:COUNT] = offset(jnp.where(low >= BIG, 0, low))
    mine = jnp.sum(jnp.where(unit == me, perm, 0), axis=1, keepdims=True)
    local = mine - unit * ROWS
    for r, low in extract(jnp.where((local >= 0) & (local < ROWS), local * 256 + row, BIG)):
        takes_ref[r : r + 1, 0:COUNT] = offset(jnp.where(low >= BIG, ROWS, low & 255))


def row_at(start):
    return pl.ds(start, TALL, stride=8)


def cell(at, r):
    return slice(at * CELL + r * TALL, at * CELL + r * TALL + TALL)


def pack(sends_ref, rows_ref, block, units):
    for at, unit in enumerate(units):
        for r in range(LIMIT):
            block[cell(at, r), :] = rows_ref[row_at(sends_ref[r, unit]), :]


def pack_by_z_kernel(sends_ref, rows_ref, *blocks):
    for dz, block in zip(Z_ORDER + (0,), blocks):
        pack(sends_ref, rows_ref, block, [unit_at(line, dz, 1) for line in range(LINES)])


def pack_by_line_kernel(sends_ref, rows_ref, *blocks):
    for line, block in zip(LINE_ORDER + (0,), blocks):
        pack(sends_ref, rows_ref, block, [unit_at(line, dz, 1) for dz in range(NZ)])


def turn_kernel(*refs):
    sources, targets = refs[:8], refs[-8:]
    for i in range(8):
        for j in range(8):
            targets[j][i * CELL : (i + 1) * CELL, :] = sources[i][j * CELL : (j + 1) * CELL, :]


def merge(takes_ref, own_ref, block, merged, units):
    for at, unit in enumerate(units):
        for r in range(LIMIT):
            start = takes_ref[r, unit]
            own = own_ref[row_at(jnp.where(start < FLAT, start, 0)), :]
            merged[row_at(start), :] = (own + block[cell(at, r), :]) * 0.5


def store(merged, out_ref, sem):
    copy = pltpu.make_async_copy(merged.at[0:FLAT], out_ref, sem)
    copy.start()
    copy.wait()


def unpack_by_line_kernel(takes_ref, own_ref, *refs):
    blocks, (out_ref, merged, sem) = refs[:LINES], refs[LINES:]
    for line, block in enumerate(blocks):
        merge(takes_ref, own_ref, block, merged, [unit_at(line, dz, -1) for dz in range(NZ)])
    store(merged, out_ref, sem)


def unpack_early_kernel(shifts, takes_ref, own_ref, *refs):
    blocks, merged = refs[:-1], refs[-1]
    for dz, block in zip(shifts, blocks):
        merge(takes_ref, own_ref, block, merged, [unit_at(line, dz, -1) for line in range(LINES)])


def unpack_late_kernel(shifts, takes_ref, own_ref, early_ref, *refs):
    blocks, (out_ref, merged, sem) = refs[: len(shifts)], refs[len(shifts) :]
    merged[...] = early_ref[...]
    for dz, block in zip(shifts, blocks):
        merge(takes_ref, own_ref, block, merged, [unit_at(line, dz, -1) for line in range(LINES)])
    store(merged, out_ref, sem)


def tiles_of(x):
    return x.reshape(ROWS // 8, 8, TALL, 128).transpose(0, 2, 1, 3).reshape(FLAT, 128)


def rows_of(x):
    return x.reshape(ROWS // 8, TALL, 8, 128).transpose(0, 2, 1, 3).reshape(ROWS, WIDTH)


def sent(block, dx, dz, dc):
    def at(x, z, c):
        return (x % NX * NZ + z % NZ) * NC + c % NC

    pairs = [
        (at(x, z, c), at(x + dx, z + dz, c + dc)) for x in range(NX) for z in range(NZ) for c in range(NC)
    ]
    return lax.ppermute(block, UNITS, pairs)


def in_order(blocks, order):
    return [blocks[-1]] + [blocks[order.index(i)] for i in range(1, 8)]


def by_z(blocks):
    blocks = list(blocks)
    for dz in Z_ORDER:
        blocks[dz] = sent(blocks[dz], 0, dz, 0)
    return blocks


def by_line(blocks):
    blocks = list(blocks)
    for line in LINE_ORDER:
        blocks[line] = sent(blocks[line], line >> 1, 0, line & 1)
    return blocks


VMEM = pl.BlockSpec(memory_space=pltpu.VMEM)
SMEM = pl.BlockSpec(memory_space=pltpu.SMEM)
HBM = pl.BlockSpec(memory_space=pltpu.HBM)
PACKED = (jax.ShapeDtypeStruct((BLOCK, 128), jnp.float32),) * 8
MERGED = (FLAT + 8 * TALL, 128)
SCRATCH = [pltpu.VMEM(MERGED, jnp.float32), pltpu.SemaphoreType.DMA]


def call(kernel, out, specs, out_specs, scratch=(), flops=500_000_000):
    return pl.pallas_call(
        kernel,
        out_shape=out,
        in_specs=specs,
        out_specs=out_specs,
        scratch_shapes=list(scratch),
        cost_estimate=pl.CostEstimate(flops=flops, bytes_accessed=1 << 20, transcendentals=0),
        compiler_params=pltpu.CompilerParams(vmem_limit_bytes=12 << 20),
    )


def on_device(a_up, a_down, b_up, b_down, perm):
    out = jax.ShapeDtypeStruct((FLAT, 128), jnp.float32)
    table = jax.ShapeDtypeStruct((8, 128), jnp.int32)
    sends, takes = call(tables_kernel, (table, table), [VMEM], (VMEM, VMEM), flops=2_000_000_000)(
        perm.reshape(COUNT, ROWS).T
    )
    down = call(pack_by_z_kernel, PACKED, [SMEM, VMEM], (VMEM,) * 8)(sends, tiles_of(b_down))
    down = by_z(in_order(down, Z_ORDER))
    up = call(pack_by_line_kernel, PACKED, [SMEM, VMEM], (VMEM,) * 8)(sends, tiles_of(b_up))
    up = by_line(in_order(up, LINE_ORDER))
    up = call(turn_kernel, PACKED, [VMEM] * 8, (VMEM,) * 8)(*up)
    up = by_z(up)
    down = call(turn_kernel, PACKED, [VMEM] * 8, (VMEM,) * 8)(*down)
    down = by_line(down)
    merged_down = call(
        unpack_by_line_kernel, out, [SMEM, VMEM] + [VMEM] * LINES, HBM, SCRATCH
    )(takes, tiles_of(a_down), *down)
    late = Z_ORDER[-2:]
    early = (0,) + Z_ORDER[:-2]
    own = tiles_of(a_up)
    merged_up = call(
        functools.partial(unpack_early_kernel, early),
        jax.ShapeDtypeStruct(MERGED, jnp.float32),
        [SMEM, VMEM] + [VMEM] * len(early),
        VMEM,
    )(takes, own, *[up[dz] for dz in early])
    merged_up = call(
        functools.partial(unpack_late_kernel, late), out, [SMEM, VMEM, VMEM] + [VMEM] * len(late), HBM, SCRATCH
    )(takes, own, merged_up, *[up[dz] for dz in late])
    return rows_of(merged_up), rows_of(merged_down)


def solution(mesh):
    finer = Mesh(
        mesh.devices.reshape(NX, NZ, NC, mesh.shape["expert"]),
        ("units_0", "units_1", "units_2", "expert"),
    )
    rows = P(EXPERT_UNITS, None)
    return jax.shard_map(
        on_device,
        mesh=finer,
        in_specs=(rows, rows, rows, rows, P("expert")),
        out_specs=(rows, rows),
        check_vma=False,
    )
```

```python
import functools

import jax
import jax.numpy as jnp
from jax import lax
from jax.experimental import pallas as pl
from jax.experimental.pallas import tpu as pltpu
from jax.sharding import Mesh
from jax.sharding import PartitionSpec as P


UNITS = ("units_0", "units_1", "units_2")
EXPERT_UNITS = ("expert", "units_0", "units_1", "units_2")
NX, NZ, NC = 4, 8, 2
COUNT = NX * NZ * NC
LINES = NX * NC
ROWS = 224
LIMIT = 5
WIDTH = 2048
TALL = WIDTH // 128
FLAT = ROWS * TALL
CELL = LIMIT * TALL
BLOCK = LINES * CELL
BIG = 1 << 24
Z_ORDER = (4, 3, 5, 2, 6, 1, 7)
Z_LAST = (1, 7, 2, 6, 3, 5, 4)
LINE_ORDER = (4, 2, 6, 5, 3, 7, 1)


def unit_at(line, dz, sign):
    x = (lax.axis_index("units_0") + sign * (line >> 1)) & (NX - 1)
    z = (lax.axis_index("units_1") + sign * dz) & (NZ - 1)
    c = (lax.axis_index("units_2") + sign * (line & 1)) & (NC - 1)
    return (x * NZ + z) * NC + c


def offset(row):
    return (row >> 3) * (8 * TALL) + (row & 7)


def extract(keys):
    for r in range(LIMIT):
        low = jnp.min(keys, axis=0, keepdims=True)
        yield r, low
        keys = jnp.where(keys == low, BIG, keys)


def by_target(perm):
    lines = COUNT * ROWS // 128
    line = lax.broadcasted_iota(jnp.int32, (lines, COUNT), 0)
    first = (lax.broadcasted_iota(jnp.int32, (lines, COUNT), 1) * ROWS) >> 7
    high = (perm >> 7).astype(jnp.float32)
    low = (perm & 127).astype(jnp.float32)
    parts = []
    for k in range(3):
        pick = jnp.where(line == first + k, 1.0, 0.0)
        high_k, low_k = (
            lax.dot_general(x, pick, (((0,), (0,)), ((), ())), preferred_element_type=jnp.float32)
            for x in (high, low)
        )
        parts.append(high_k.astype(jnp.int32) * 128 + low_k.astype(jnp.int32))
    whole = jnp.concatenate(parts, axis=0)
    skip = (lax.broadcasted_iota(jnp.int32, whole.shape, 1) * ROWS) & 127
    row = lax.broadcasted_iota(jnp.int32, whole.shape, 0) - skip
    return jnp.where((row >= 0) & (row < ROWS), whole, -1), row


def tables_kernel(perm_ref, sends_ref, takes_ref):
    me = lax.axis_index(UNITS)
    perm, row = by_target(perm_ref[...])
    unit = lax.broadcasted_iota(jnp.int32, perm.shape, 1)
    local = perm - me * ROWS
    for r, low in extract(jnp.where((local >= 0) & (local < ROWS), local, BIG)):
        sends_ref[r : r + 1, 0:COUNT] = offset(jnp.where(low >= BIG, 0, low))
    mine = jnp.sum(jnp.where(unit == me, perm, 0), axis=1, keepdims=True)
    row = jnp.sum(jnp.where(unit == me, row, 0), axis=1, keepdims=True)
    local = mine - unit * ROWS
    for r, low in extract(jnp.where((local >= 0) & (local < ROWS), local * 256 + row, BIG)):
        takes_ref[r : r + 1, 0:COUNT] = offset(jnp.where(low >= BIG, ROWS, low & 255))


def row_at(start):
    return pl.ds(start, TALL, stride=8)


def cell(at, r):
    return slice(at * CELL + r * TALL, at * CELL + r * TALL + TALL)


def pack(sends_ref, rows_ref, block, units):
    for at, unit in enumerate(units):
        for r in range(LIMIT):
            block[cell(at, r), :] = rows_ref[row_at(sends_ref[r, unit]), :]


def pack_by_z_kernel(shifts, sends_ref, rows_ref, *blocks):
    for dz, block in zip(shifts, blocks):
        pack(sends_ref, rows_ref, block, [unit_at(line, dz, 1) for line in range(LINES)])


def pack_by_line_kernel(sends_ref, rows_ref, *blocks):
    for line, block in zip(LINE_ORDER + (0,), blocks):
        pack(sends_ref, rows_ref, block, [unit_at(line, dz, 1) for dz in range(NZ)])


def turn_kernel(*refs):
    sources, targets = refs[:8], refs[-8:]
    for i in range(8):
        for j in range(8):
            targets[j][i * CELL : (i + 1) * CELL, :] = sources[i][j * CELL : (j + 1) * CELL, :]


def merge(takes_ref, own_ref, block, merged, units):
    for at, unit in enumerate(units):
        for r in range(LIMIT):
            start = takes_ref[r, unit]
            own = own_ref[row_at(jnp.where(start < FLAT, start, 0)), :]
            merged[row_at(start), :] = (own + block[cell(at, r), :]) * 0.5


def store(merged, out_ref, sem):
    copy = pltpu.make_async_copy(merged.at[0:FLAT], out_ref, sem)
    copy.start()
    copy.wait()


def unpack_by_line_kernel(takes_ref, own_ref, *refs):
    blocks, (out_ref, merged, sem) = refs[:LINES], refs[LINES:]
    for line, block in enumerate(blocks):
        merge(takes_ref, own_ref, block, merged, [unit_at(line, dz, -1) for dz in range(NZ)])
    store(merged, out_ref, sem)


def unpack_early_kernel(shifts, takes_ref, own_ref, *refs):
    blocks, merged = refs[:-1], refs[-1]
    for dz, block in zip(shifts, blocks):
        merge(takes_ref, own_ref, block, merged, [unit_at(line, dz, -1) for line in range(LINES)])


def unpack_late_kernel(shifts, takes_ref, own_ref, early_ref, *refs):
    blocks, (out_ref, merged, sem) = refs[: len(shifts)], refs[len(shifts) :]
    merged[...] = early_ref[...]
    for dz, block in zip(shifts, blocks):
        merge(takes_ref, own_ref, block, merged, [unit_at(line, dz, -1) for line in range(LINES)])
    store(merged, out_ref, sem)


def tiles_of(x):
    return x.reshape(ROWS // 8, 8, TALL, 128).transpose(0, 2, 1, 3).reshape(FLAT, 128)


def rows_of(x):
    return x.reshape(ROWS // 8, TALL, 8, 128).transpose(0, 2, 1, 3).reshape(ROWS, WIDTH)


def sent(block, dx, dz, dc):
    def at(x, z, c):
        return (x % NX * NZ + z % NZ) * NC + c % NC

    pairs = [
        (at(x, z, c), at(x + dx, z + dz, c + dc)) for x in range(NX) for z in range(NZ) for c in range(NC)
    ]
    return lax.ppermute(block, UNITS, pairs)


def in_order(blocks, order):
    return [blocks[-1]] + [blocks[order.index(i)] for i in range(1, 8)]


def by_z(blocks, order):
    blocks = list(blocks)
    for dz in order:
        blocks[dz] = sent(blocks[dz], 0, dz, 0)
    return blocks


def by_line(blocks):
    blocks = list(blocks)
    for line in LINE_ORDER:
        blocks[line] = sent(blocks[line], line >> 1, 0, line & 1)
    return blocks


VMEM = pl.BlockSpec(memory_space=pltpu.VMEM)
SMEM = pl.BlockSpec(memory_space=pltpu.SMEM)
HBM = pl.BlockSpec(memory_space=pltpu.HBM)
PACKED = (jax.ShapeDtypeStruct((BLOCK, 128), jnp.float32),) * 8
MERGED = (FLAT + 8 * TALL, 128)
SCRATCH = [pltpu.VMEM(MERGED, jnp.float32), pltpu.SemaphoreType.DMA]


def call(kernel, out, specs, out_specs, scratch=(), flops=500_000_000):
    return pl.pallas_call(
        kernel,
        out_shape=out,
        in_specs=specs,
        out_specs=out_specs,
        scratch_shapes=list(scratch),
        cost_estimate=pl.CostEstimate(flops=flops, bytes_accessed=1 << 20, transcendentals=0),
        compiler_params=pltpu.CompilerParams(vmem_limit_bytes=12 << 20),
    )


def on_device(a_up, a_down, b_up, b_down, perm):
    out = jax.ShapeDtypeStruct((FLAT, 128), jnp.float32)
    table = jax.ShapeDtypeStruct((8, 128), jnp.int32)
    sends, takes = call(tables_kernel, (table, table), [VMEM], (VMEM, VMEM), flops=2_000_000_000)(
        perm.reshape(COUNT * ROWS // 128, 128)
    )
    down = []
    for shifts in (Z_ORDER[:2], Z_ORDER[2:] + (0,)):
        down += call(
            functools.partial(pack_by_z_kernel, shifts), PACKED[: len(shifts)], [SMEM, VMEM], (VMEM,) * len(shifts)
        )(sends, tiles_of(b_down))
    down = by_z(in_order(down, Z_ORDER), Z_ORDER)
    up = call(pack_by_line_kernel, PACKED, [SMEM, VMEM], (VMEM,) * 8)(sends, tiles_of(b_up))
    up = by_line(in_order(up, LINE_ORDER))
    up = call(turn_kernel, PACKED, [VMEM] * 8, (VMEM,) * 8)(*up)
    up = by_z(up, Z_LAST)
    down = call(turn_kernel, PACKED, [VMEM] * 8, (VMEM,) * 8)(*down)
    down = by_line(down)
    merged_down = call(
        unpack_by_line_kernel, out, [SMEM, VMEM] + [VMEM] * LINES, HBM, SCRATCH
    )(takes, tiles_of(a_down), *down)
    late = Z_LAST[-2:]
    early = (0,) + Z_LAST[:-2]
    own = tiles_of(a_up)
    merged_up = call(
        functools.partial(unpack_early_kernel, early),
        jax.ShapeDtypeStruct(MERGED, jnp.float32),
        [SMEM, VMEM] + [VMEM] * len(early),
        VMEM,
    )(takes, own, *[up[dz] for dz in early])
    merged_up = call(
        functools.partial(unpack_late_kernel, late), out, [SMEM, VMEM, VMEM] + [VMEM] * len(late), HBM, SCRATCH
    )(takes, own, merged_up, *[up[dz] for dz in late])
    return rows_of(merged_up), rows_of(merged_down)


def solution(mesh):
    finer = Mesh(
        mesh.devices.reshape(NX, NZ, NC, mesh.shape["expert"]),
        ("units_0", "units_1", "units_2", "expert"),
    )
    rows = P(EXPERT_UNITS, None)
    return jax.shard_map(
        on_device,
        mesh=finer,
        in_specs=(rows, rows, rows, rows, P("expert")),
        out_specs=(rows, rows),
        check_vma=False,
    )
```

```python
import functools

import jax
import jax.numpy as jnp
from jax import lax
from jax.experimental import pallas as pl
from jax.experimental.pallas import tpu as pltpu
from jax.sharding import Mesh
from jax.sharding import PartitionSpec as P


UNITS = ("units_0", "units_1", "units_2")
EXPERT_UNITS = ("expert", "units_0", "units_1", "units_2")
NX, NZ, NC = 4, 8, 2
COUNT = NX * NZ * NC
LINES = NX * NC
ROWS = 224
LIMIT = 5
WIDTH = 2048
TALL = WIDTH // 128
FLAT = ROWS * TALL
CELL = LIMIT * TALL
BLOCK = LINES * CELL
BIG = 1 << 24
STORES = 4
Z_ORDER = (4, 3, 5, 2, 6, 1, 7)
Z_LAST = (2, 6, 1, 7, 3, 5, 4)
LINE_ORDER = (4, 2, 6, 5, 3, 7, 1)


def unit_at(line, dz, sign):
    x = (lax.axis_index("units_0") + sign * (line >> 1)) & (NX - 1)
    z = (lax.axis_index("units_1") + sign * dz) & (NZ - 1)
    c = (lax.axis_index("units_2") + sign * (line & 1)) & (NC - 1)
    return (x * NZ + z) * NC + c


def offset(row):
    return (row >> 3) * (8 * TALL) + (row & 7)


def extract(keys):
    for r in range(LIMIT):
        low = jnp.min(keys, axis=0, keepdims=True)
        yield r, low
        keys = jnp.where(keys == low, BIG, keys)


def by_target(high, low):
    lines = high.shape[0]
    line = lax.broadcasted_iota(jnp.int32, (lines, COUNT), 0)
    first = (lax.broadcasted_iota(jnp.int32, (lines, COUNT), 1) * ROWS) >> 7
    parts = []
    for k in range(3):
        pick = jnp.where(line == first + k, 1.0, 0.0)
        high_k, low_k = (
            lax.dot_general(x, pick, (((0,), (0,)), ((), ())), preferred_element_type=jnp.float32)
            for x in (high, low)
        )
        parts.append(high_k.astype(jnp.int32) * 128 + low_k.astype(jnp.int32))
    whole = jnp.concatenate(parts, axis=0)
    skip = (lax.broadcasted_iota(jnp.int32, whole.shape, 1) * ROWS) & 127
    row = lax.broadcasted_iota(jnp.int32, whole.shape, 0) - skip
    return jnp.where((row >= 0) & (row < ROWS), whole, -1), row


def tables_kernel(high_ref, low_ref, sends_ref, takes_ref):
    me = lax.axis_index(UNITS)
    perm, row = by_target(high_ref[...], low_ref[...])
    unit = lax.broadcasted_iota(jnp.int32, perm.shape, 1)
    local = perm - me * ROWS
    for r, low in extract(jnp.where((local >= 0) & (local < ROWS), local, BIG)):
        sends_ref[r : r + 1, 0:COUNT] = offset(jnp.where(low >= BIG, 0, low))
    mine = jnp.sum(jnp.where(unit == me, perm, 0), axis=1, keepdims=True)
    row = jnp.sum(jnp.where(unit == me, row, 0), axis=1, keepdims=True)
    local = mine - unit * ROWS
    for r, low in extract(jnp.where((local >= 0) & (local < ROWS), local * 256 + row, BIG)):
        takes_ref[r : r + 1, 0:COUNT] = offset(jnp.where(low >= BIG, ROWS, low & 255))


def row_at(start):
    return pl.ds(start, TALL, stride=8)


def cell(at, r):
    return slice(at * CELL + r * TALL, at * CELL + r * TALL + TALL)


def pack(sends_ref, rows_ref, block, units):
    for at, unit in enumerate(units):
        for r in range(LIMIT):
            block[cell(at, r), :] = rows_ref[row_at(sends_ref[r, unit]), :]


def pack_by_z_kernel(shifts, sends_ref, rows_ref, *blocks):
    for dz, block in zip(shifts, blocks):
        pack(sends_ref, rows_ref, block, [unit_at(line, dz, 1) for line in range(LINES)])


def pack_by_line_kernel(sends_ref, rows_ref, *blocks):
    for line, block in zip(LINE_ORDER + (0,), blocks):
        pack(sends_ref, rows_ref, block, [unit_at(line, dz, 1) for dz in range(NZ)])


def turn_kernel(*refs):
    sources, targets = refs[:8], refs[-8:]
    for i in range(8):
        for j in range(8):
            targets[j][i * CELL : (i + 1) * CELL, :] = sources[i][j * CELL : (j + 1) * CELL, :]


def merge(takes_ref, own_ref, block, merged, units):
    for at, unit in enumerate(units):
        for r in range(LIMIT):
            start = takes_ref[r, unit]
            own = own_ref[row_at(jnp.where(start < FLAT, start, 0)), :]
            merged[row_at(start), :] = (own + block[cell(at, r), :]) * 0.5


def store(merged, out_ref, sems):
    part = FLAT // STORES
    copies = [
        pltpu.make_async_copy(merged.at[pl.ds(i * part, part)], out_ref.at[pl.ds(i * part, part)], sems.at[i])
        for i in range(STORES)
    ]
    for copy in copies:
        copy.start()
    for copy in copies:
        copy.wait()


def unpack_by_line_kernel(takes_ref, own_ref, *refs):
    blocks, (out_ref, merged, sem) = refs[:LINES], refs[LINES:]
    for line, block in enumerate(blocks):
        merge(takes_ref, own_ref, block, merged, [unit_at(line, dz, -1) for dz in range(NZ)])
    store(merged, out_ref, sem)


def unpack_early_kernel(shifts, takes_ref, own_ref, *refs):
    blocks, merged = refs[:-1], refs[-1]
    for dz, block in zip(shifts, blocks):
        merge(takes_ref, own_ref, block, merged, [unit_at(line, dz, -1) for line in range(LINES)])


def unpack_late_kernel(shifts, takes_ref, own_ref, early_ref, *refs):
    blocks, (out_ref, merged, sem) = refs[: len(shifts)], refs[len(shifts) :]
    for dz, block in zip(shifts, blocks):
        merge(takes_ref, own_ref, block, merged, [unit_at(line, dz, -1) for line in range(LINES)])
    store(merged, out_ref, sem)


def tiles_of(x):
    return x.reshape(ROWS // 8, 8, TALL, 128).transpose(0, 2, 1, 3).reshape(FLAT, 128)


def rows_of(x):
    return x.reshape(ROWS // 8, TALL, 8, 128).transpose(0, 2, 1, 3).reshape(ROWS, WIDTH)


def sent(block, dx, dz, dc):
    def at(x, z, c):
        return (x % NX * NZ + z % NZ) * NC + c % NC

    pairs = [
        (at(x, z, c), at(x + dx, z + dz, c + dc)) for x in range(NX) for z in range(NZ) for c in range(NC)
    ]
    return lax.ppermute(block, UNITS, pairs)


def in_order(blocks, order):
    return [blocks[-1]] + [blocks[order.index(i)] for i in range(1, 8)]


def by_z(blocks, order):
    blocks = list(blocks)
    for dz in order:
        blocks[dz] = sent(blocks[dz], 0, dz, 0)
    return blocks


def by_line(blocks):
    blocks = list(blocks)
    for line in LINE_ORDER:
        blocks[line] = sent(blocks[line], line >> 1, 0, line & 1)
    return blocks


VMEM = pl.BlockSpec(memory_space=pltpu.VMEM)
SMEM = pl.BlockSpec(memory_space=pltpu.SMEM)
HBM = pl.BlockSpec(memory_space=pltpu.HBM)
PACKED = (jax.ShapeDtypeStruct((BLOCK, 128), jnp.float32),) * 8
MERGED = (FLAT + 8 * TALL, 128)
SEMS = pltpu.SemaphoreType.DMA((STORES,))
SCRATCH = [pltpu.VMEM(MERGED, jnp.float32), SEMS]


def call(kernel, out, specs, out_specs, scratch=(), flops=500_000_000, aliases=None):
    return pl.pallas_call(
        kernel,
        out_shape=out,
        in_specs=specs,
        out_specs=out_specs,
        scratch_shapes=list(scratch),
        input_output_aliases=aliases or {},
        cost_estimate=pl.CostEstimate(flops=flops, bytes_accessed=1 << 20, transcendentals=0),
        compiler_params=pltpu.CompilerParams(vmem_limit_bytes=12 << 20),
    )


def on_device(a_up, a_down, b_up, b_down, perm):
    out = jax.ShapeDtypeStruct((FLAT, 128), jnp.float32)
    table = jax.ShapeDtypeStruct((8, 128), jnp.int32)
    perm = perm.reshape(COUNT * ROWS // 128, 128)
    sends, takes = call(tables_kernel, (table, table), [VMEM, VMEM], (VMEM, VMEM), flops=700_000_000)(
        (perm >> 7).astype(jnp.float32), (perm & 127).astype(jnp.float32)
    )
    down = []
    for shifts in (Z_ORDER[:1], Z_ORDER[1:] + (0,)):
        down += call(
            functools.partial(pack_by_z_kernel, shifts), PACKED[: len(shifts)], [SMEM, VMEM], (VMEM,) * len(shifts)
        )(sends, tiles_of(b_down))
    down = by_z(in_order(down, Z_ORDER), Z_ORDER)
    up = call(pack_by_line_kernel, PACKED, [SMEM, VMEM], (VMEM,) * 8)(sends, tiles_of(b_up))
    up = by_line(in_order(up, LINE_ORDER))
    up = call(turn_kernel, PACKED, [VMEM] * 8, (VMEM,) * 8)(*up)
    up = by_z(up, Z_LAST)
    down = call(turn_kernel, PACKED, [VMEM] * 8, (VMEM,) * 8)(*down)
    down = by_line(down)
    merged_down = call(
        unpack_by_line_kernel, out, [SMEM, VMEM] + [VMEM] * LINES, HBM, SCRATCH
    )(takes, tiles_of(a_down), *down)
    late = Z_LAST[-1:]
    early = (0,) + Z_LAST[:-1]
    own = tiles_of(a_up)
    merged_up = call(
        functools.partial(unpack_early_kernel, early),
        jax.ShapeDtypeStruct(MERGED, jnp.float32),
        [SMEM, VMEM] + [VMEM] * len(early),
        VMEM,
    )(takes, own, *[up[dz] for dz in early])
    merged_up, _ = call(
        functools.partial(unpack_late_kernel, late),
        (out, jax.ShapeDtypeStruct(MERGED, jnp.float32)),
        [SMEM, VMEM, VMEM] + [VMEM] * len(late),
        (HBM, VMEM),
        [SEMS],
        aliases={2: 1},
    )(takes, own, merged_up, *[up[dz] for dz in late])
    return rows_of(merged_up), rows_of(merged_down)


def solution(mesh):
    finer = Mesh(
        mesh.devices.reshape(NX, NZ, NC, mesh.shape["expert"]),
        ("units_0", "units_1", "units_2", "expert"),
    )
    rows = P(EXPERT_UNITS, None)
    return jax.shard_map(
        on_device,
        mesh=finer,
        in_specs=(rows, rows, rows, rows, P("expert")),
        out_specs=(rows, rows),
        check_vma=False,
    )
```

```python
import functools

import jax
import jax.numpy as jnp
from jax import lax
from jax.experimental import pallas as pl
from jax.experimental.pallas import tpu as pltpu
from jax.sharding import Mesh
from jax.sharding import PartitionSpec as P


UNITS = ("units_0", "units_1", "units_2")
EXPERT_UNITS = ("expert", "units_0", "units_1", "units_2")
NX, NZ, NC = 4, 8, 2
COUNT = NX * NZ * NC
LINES = NX * NC
ROWS = 224
LIMIT = 5
WIDTH = 2048
TALL = WIDTH // 128
FLAT = ROWS * TALL
CELL = LIMIT * TALL
BLOCK = LINES * CELL
BIG = 1 << 24
STORES = 4
Z_ORDER = (4, 3, 5, 2, 6, 1, 7)
Z_LAST = (2, 6, 1, 7, 3, 5, 4)
LINE_ORDER = (4, 2, 6, 5, 3, 7, 1)
LAST = Z_LAST[-1]
EARLY = (0,) + Z_LAST[:-1]
HALF = TALL // 2


def unit_at(line, dz, sign):
    x = (lax.axis_index("units_0") + sign * (line >> 1)) & (NX - 1)
    z = (lax.axis_index("units_1") + sign * dz) & (NZ - 1)
    c = (lax.axis_index("units_2") + sign * (line & 1)) & (NC - 1)
    return (x * NZ + z) * NC + c


def offset(row):
    return (row >> 3) * (8 * TALL) + (row & 7)


def extract(keys):
    for r in range(LIMIT):
        low = jnp.min(keys, axis=0, keepdims=True)
        yield r, low
        keys = jnp.where(keys == low, BIG, keys)


def by_target(high, low):
    lines = high.shape[0]
    line = lax.broadcasted_iota(jnp.int32, (lines, COUNT), 0)
    first = (lax.broadcasted_iota(jnp.int32, (lines, COUNT), 1) * ROWS) >> 7
    parts = []
    for k in range(3):
        pick = jnp.where(line == first + k, 1.0, 0.0)
        high_k, low_k = (
            lax.dot_general(x, pick, (((0,), (0,)), ((), ())), preferred_element_type=jnp.float32)
            for x in (high, low)
        )
        parts.append(high_k.astype(jnp.int32) * 128 + low_k.astype(jnp.int32))
    whole = jnp.concatenate(parts, axis=0)
    skip = (lax.broadcasted_iota(jnp.int32, whole.shape, 1) * ROWS) & 127
    row = lax.broadcasted_iota(jnp.int32, whole.shape, 0) - skip
    return jnp.where((row >= 0) & (row < ROWS), whole, -1), row


def tables_kernel(high_ref, low_ref, sends_ref, takes_ref):
    me = lax.axis_index(UNITS)
    perm, row = by_target(high_ref[...], low_ref[...])
    unit = lax.broadcasted_iota(jnp.int32, perm.shape, 1)
    local = perm - me * ROWS
    for r, low in extract(jnp.where((local >= 0) & (local < ROWS), local, BIG)):
        sends_ref[r : r + 1, 0:COUNT] = offset(jnp.where(low >= BIG, 0, low))
    mine = jnp.sum(jnp.where(unit == me, perm, 0), axis=1, keepdims=True)
    row = jnp.sum(jnp.where(unit == me, row, 0), axis=1, keepdims=True)
    local = mine - unit * ROWS
    for r, low in extract(jnp.where((local >= 0) & (local < ROWS), local * 256 + row, BIG)):
        takes_ref[r : r + 1, 0:COUNT] = offset(jnp.where(low >= BIG, ROWS, low & 255))


def row_at(start):
    return pl.ds(start, TALL, stride=8)


def cell(at, r):
    return slice(at * CELL + r * TALL, at * CELL + r * TALL + TALL)


def half_cell(at, r):
    return slice((at * LIMIT + r) * HALF, (at * LIMIT + r + 1) * HALF)


def pack(sends_ref, rows_ref, block, units):
    for at, unit in enumerate(units):
        for r in range(LIMIT):
            block[cell(at, r), :] = rows_ref[row_at(sends_ref[r, unit]), :]


def pack_by_z_kernel(shifts, sends_ref, rows_ref, *blocks):
    for dz, block in zip(shifts, blocks):
        pack(sends_ref, rows_ref, block, [unit_at(line, dz, 1) for line in range(LINES)])


def pack_by_line_kernel(sends_ref, rows_ref, *blocks):
    for line, block in zip(LINE_ORDER + (0,), blocks):
        pack(sends_ref, rows_ref, block, [unit_at(line, dz, 1) for dz in range(NZ)])


def turn_kernel(*refs):
    sources, targets = refs[:8], refs[-8:]
    for i in range(8):
        for j in range(8):
            targets[j][i * CELL : (i + 1) * CELL, :] = sources[i][j * CELL : (j + 1) * CELL, :]


def turn_split_kernel(*refs):
    sources, targets, halves = refs[:8], refs[8:15], refs[15:]
    for i in range(8):
        for target, j in zip(targets, EARLY):
            target[i * CELL : (i + 1) * CELL, :] = sources[i][j * CELL : (j + 1) * CELL, :]
        for r in range(LIMIT):
            for side, half in enumerate(halves):
                at = LAST * CELL + r * TALL + side * HALF
                half[half_cell(i, r), :] = sources[i][at : at + HALF, :]


def merge(takes_ref, own_ref, block, merged, units):
    for at, unit in enumerate(units):
        for r in range(LIMIT):
            start = takes_ref[r, unit]
            own = own_ref[row_at(jnp.where(start < FLAT, start, 0)), :]
            merged[row_at(start), :] = (own + block[cell(at, r), :]) * 0.5


def store(merged, out_ref, sems):
    part = FLAT // STORES
    copies = [
        pltpu.make_async_copy(merged.at[pl.ds(i * part, part)], out_ref.at[pl.ds(i * part, part)], sems.at[i])
        for i in range(STORES)
    ]
    for copy in copies:
        copy.start()
    for copy in copies:
        copy.wait()


def unpack_by_line_kernel(takes_ref, own_ref, *refs):
    blocks, (out_ref, merged, sem) = refs[:LINES], refs[LINES:]
    for line, block in enumerate(blocks):
        merge(takes_ref, own_ref, block, merged, [unit_at(line, dz, -1) for dz in range(NZ)])
    store(merged, out_ref, sem)


def unpack_early_kernel(shifts, takes_ref, own_ref, *refs):
    blocks, merged = refs[:-1], refs[-1]
    for dz, block in zip(shifts, blocks):
        merge(takes_ref, own_ref, block, merged, [unit_at(line, dz, -1) for line in range(LINES)])


def unpack_half_kernel(side, takes_ref, own_ref, early_ref, block, *refs):
    out_ref, merged, sems = refs[-3:]
    shift = side * HALF * 8
    for line in range(LINES):
        unit = unit_at(line, LAST, -1)
        for r in range(LIMIT):
            start = takes_ref[r, unit]
            own = own_ref[pl.ds(jnp.where(start < FLAT, start, 0) + shift, HALF, stride=8), :]
            merged[pl.ds(start + shift, HALF, stride=8), :] = (own + block[half_cell(line, r), :]) * 0.5
    copies = []
    for group in range(ROWS // 8):
        rows = pl.ds(group * 8 * TALL + shift, 8 * HALF)
        copies.append(pltpu.make_async_copy(merged.at[rows], out_ref.at[rows], sems.at[group]))
        copies[-1].start()
    for copy in copies:
        copy.wait()


def tiles_of(x):
    return x.reshape(ROWS // 8, 8, TALL, 128).transpose(0, 2, 1, 3).reshape(FLAT, 128)


def rows_of(x):
    return x.reshape(ROWS // 8, TALL, 8, 128).transpose(0, 2, 1, 3).reshape(ROWS, WIDTH)


def sent(block, dx, dz, dc):
    def at(x, z, c):
        return (x % NX * NZ + z % NZ) * NC + c % NC

    pairs = [
        (at(x, z, c), at(x + dx, z + dz, c + dc)) for x in range(NX) for z in range(NZ) for c in range(NC)
    ]
    return lax.ppermute(block, UNITS, pairs)


def in_order(blocks, order):
    return [blocks[-1]] + [blocks[order.index(i)] for i in range(1, 8)]


def by_z(blocks, order):
    blocks = dict(blocks) if isinstance(blocks, dict) else list(blocks)
    for dz in order:
        blocks[dz] = sent(blocks[dz], 0, dz, 0)
    return blocks


def by_line(blocks):
    blocks = list(blocks)
    for line in LINE_ORDER:
        blocks[line] = sent(blocks[line], line >> 1, 0, line & 1)
    return blocks


VMEM = pl.BlockSpec(memory_space=pltpu.VMEM)
SMEM = pl.BlockSpec(memory_space=pltpu.SMEM)
HBM = pl.BlockSpec(memory_space=pltpu.HBM)
PACKED = (jax.ShapeDtypeStruct((BLOCK, 128), jnp.float32),) * 8
MERGED = (FLAT + 8 * TALL, 128)
SEMS = pltpu.SemaphoreType.DMA((STORES,))
SCRATCH = [pltpu.VMEM(MERGED, jnp.float32), SEMS]


def call(kernel, out, specs, out_specs, scratch=(), flops=500_000_000, aliases=None):
    return pl.pallas_call(
        kernel,
        out_shape=out,
        in_specs=specs,
        out_specs=out_specs,
        scratch_shapes=list(scratch),
        input_output_aliases=aliases or {},
        cost_estimate=pl.CostEstimate(flops=flops, bytes_accessed=1 << 20, transcendentals=0),
        compiler_params=pltpu.CompilerParams(vmem_limit_bytes=12 << 20),
    )


def on_device(a_up, a_down, b_up, b_down, perm):
    out = jax.ShapeDtypeStruct((FLAT, 128), jnp.float32)
    table = jax.ShapeDtypeStruct((8, 128), jnp.int32)
    perm = perm.reshape(COUNT * ROWS // 128, 128)
    sends, takes = call(tables_kernel, (table, table), [VMEM, VMEM], (VMEM, VMEM), flops=700_000_000)(
        (perm >> 7).astype(jnp.float32), (perm & 127).astype(jnp.float32)
    )
    down = []
    for shifts in (Z_ORDER[:1], Z_ORDER[1:] + (0,)):
        down += call(
            functools.partial(pack_by_z_kernel, shifts), PACKED[: len(shifts)], [SMEM, VMEM], (VMEM,) * len(shifts)
        )(sends, tiles_of(b_down))
    down = by_z(in_order(down, Z_ORDER), Z_ORDER)
    up = call(pack_by_line_kernel, PACKED, [SMEM, VMEM], (VMEM,) * 8)(sends, tiles_of(b_up))
    up = by_line(in_order(up, LINE_ORDER))
    half = jax.ShapeDtypeStruct((BLOCK // 2, 128), jnp.float32)
    *up, left, right = call(turn_split_kernel, PACKED[:7] + (half, half), [VMEM] * 8, (VMEM,) * 9)(*up)
    up = by_z(dict(zip(EARLY, up)), EARLY[1:])
    left = sent(left, 0, LAST, 0)
    right = sent(right, 0, LAST, 0)
    down = call(turn_kernel, PACKED, [VMEM] * 8, (VMEM,) * 8)(*down)
    down = by_line(down)
    merged_down = call(
        unpack_by_line_kernel, out, [SMEM, VMEM] + [VMEM] * LINES, HBM, SCRATCH
    )(takes, tiles_of(a_down), *down)
    own = tiles_of(a_up)
    merged = jax.ShapeDtypeStruct(MERGED, jnp.float32)
    rows = call(
        functools.partial(unpack_early_kernel, EARLY), merged, [SMEM, VMEM] + [VMEM] * len(EARLY), VMEM
    )(takes, own, *[up[dz] for dz in EARLY])
    stores = [pltpu.SemaphoreType.DMA((ROWS // 8,))]
    merged_up, rows = call(
        functools.partial(unpack_half_kernel, 0),
        (out, merged),
        [SMEM, VMEM, VMEM, VMEM],
        (HBM, VMEM),
        stores,
        aliases={2: 1},
    )(takes, own, rows, left)
    merged_up, _ = call(
        functools.partial(unpack_half_kernel, 1),
        (out, merged),
        [SMEM, VMEM, VMEM, VMEM, HBM],
        (HBM, VMEM),
        stores,
        aliases={2: 1, 4: 0},
    )(takes, own, rows, right, merged_up)
    return rows_of(merged_up), rows_of(merged_down)


def solution(mesh):
    finer = Mesh(
        mesh.devices.reshape(NX, NZ, NC, mesh.shape["expert"]),
        ("units_0", "units_1", "units_2", "expert"),
    )
    rows = P(EXPERT_UNITS, None)
    return jax.shard_map(
        on_device,
        mesh=finer,
        in_specs=(rows, rows, rows, rows, P("expert")),
        out_specs=(rows, rows),
        check_vma=False,
    )
```

```python
import functools

import jax
import jax.numpy as jnp
from jax import lax
from jax.experimental import pallas as pl
from jax.experimental.pallas import tpu as pltpu
from jax.sharding import Mesh
from jax.sharding import PartitionSpec as P


UNITS = ("units_0", "units_1", "units_2")
EXPERT_UNITS = ("expert", "units_0", "units_1", "units_2")
NX, NZ, NC = 4, 8, 2
COUNT = NX * NZ * NC
LINES = NX * NC
ROWS = 224
LIMIT = 5
WIDTH = 2048
TALL = WIDTH // 128
FLAT = ROWS * TALL
CELL = LIMIT * TALL
BLOCK = LINES * CELL
BIG = 1 << 24
STORES = 4
Z_ORDER = (4, 3, 5, 2, 6, 1, 7)
Z_LAST = (2, 6, 1, 7, 3, 5, 4)
LINE_ORDER = (4, 2, 6, 5, 3, 7, 1)


def unit_at(line, dz, sign):
    x = (lax.axis_index("units_0") + sign * (line >> 1)) & (NX - 1)
    z = (lax.axis_index("units_1") + sign * dz) & (NZ - 1)
    c = (lax.axis_index("units_2") + sign * (line & 1)) & (NC - 1)
    return (x * NZ + z) * NC + c


def offset(row):
    return (row >> 3) * (8 * TALL) + (row & 7)


def extract(keys):
    for r in range(LIMIT):
        low = jnp.min(keys, axis=0, keepdims=True)
        yield r, low
        keys = jnp.where(keys == low, BIG, keys)


def by_target(high, low):
    lines = high.shape[0]
    line = lax.broadcasted_iota(jnp.int32, (lines, COUNT), 0)
    first = (lax.broadcasted_iota(jnp.int32, (lines, COUNT), 1) * ROWS) >> 7
    parts = []
    for k in range(3):
        pick = jnp.where(line == first + k, 1.0, 0.0)
        high_k, low_k = (
            lax.dot_general(x, pick, (((0,), (0,)), ((), ())), preferred_element_type=jnp.float32)
            for x in (high, low)
        )
        parts.append(high_k.astype(jnp.int32) * 128 + low_k.astype(jnp.int32))
    whole = jnp.concatenate(parts, axis=0)
    skip = (lax.broadcasted_iota(jnp.int32, whole.shape, 1) * ROWS) & 127
    row = lax.broadcasted_iota(jnp.int32, whole.shape, 0) - skip
    return jnp.where((row >= 0) & (row < ROWS), whole, -1), row


def tables_kernel(high_ref, low_ref, sends_ref, takes_ref):
    me = lax.axis_index(UNITS)
    perm, row = by_target(high_ref[...], low_ref[...])
    unit = lax.broadcasted_iota(jnp.int32, perm.shape, 1)
    local = perm - me * ROWS
    for r, low in extract(jnp.where((local >= 0) & (local < ROWS), local, BIG)):
        sends_ref[r : r + 1, 0:COUNT] = offset(jnp.where(low >= BIG, 0, low))
    mine = jnp.sum(jnp.where(unit == me, perm, 0), axis=1, keepdims=True)
    row = jnp.sum(jnp.where(unit == me, row, 0), axis=1, keepdims=True)
    local = mine - unit * ROWS
    for r, low in extract(jnp.where((local >= 0) & (local < ROWS), local * 256 + row, BIG)):
        takes_ref[r : r + 1, 0:COUNT] = offset(jnp.where(low >= BIG, ROWS, low & 255))


def row_at(start):
    return pl.ds(start, TALL, stride=8)


def cell(at, r):
    return pl.ds(pl.multiple_of(at * CELL + r * TALL, TALL), TALL)


def pack(sends_ref, rows_ref, block, units):
    for at, unit in enumerate(units):
        for r in range(LIMIT):
            block[cell(at, r), :] = rows_ref[row_at(sends_ref[r, unit]), :]


def pack_by_z_kernel(shifts, sends_ref, rows_ref, *blocks):
    if len(blocks) == 1:

        def fill(line, carry):
            unit = unit_at(line, shifts[0], 1)
            for r in range(LIMIT):
                blocks[0][cell(line, r), :] = rows_ref[row_at(sends_ref[r, unit]), :]
            return carry

        lax.fori_loop(0, LINES, fill, 0)
        return
    for dz, block in zip(shifts, blocks):
        pack(sends_ref, rows_ref, block, [unit_at(line, dz, 1) for line in range(LINES)])


def pack_by_line_kernel(sends_ref, rows_ref, *blocks):
    for line, block in zip(LINE_ORDER + (0,), blocks):
        pack(sends_ref, rows_ref, block, [unit_at(line, dz, 1) for dz in range(NZ)])


def turn_kernel(*refs):
    sources, targets = refs[:8], refs[-8:]
    for i in range(8):
        for j in range(8):
            targets[j][i * CELL : (i + 1) * CELL, :] = sources[i][j * CELL : (j + 1) * CELL, :]


def merge(takes_ref, own_ref, block, merged, units):
    for at, unit in enumerate(units):
        for r in range(LIMIT):
            start = takes_ref[r, unit]
            own = own_ref[row_at(jnp.where(start < FLAT, start, 0)), :]
            merged[row_at(start), :] = (own + block[cell(at, r), :]) * 0.5


def store(merged, out_ref, sems):
    part = FLAT // STORES
    copies = [
        pltpu.make_async_copy(merged.at[pl.ds(i * part, part)], out_ref.at[pl.ds(i * part, part)], sems.at[i])
        for i in range(STORES)
    ]
    for copy in copies:
        copy.start()
    for copy in copies:
        copy.wait()


def unpack_by_line_kernel(takes_ref, own_ref, *refs):
    blocks, (out_ref, merged, sem) = refs[:LINES], refs[LINES:]
    for line, block in enumerate(blocks):
        merge(takes_ref, own_ref, block, merged, [unit_at(line, dz, -1) for dz in range(NZ)])
    store(merged, out_ref, sem)


def unpack_early_kernel(shifts, takes_ref, own_ref, *refs):
    blocks, merged = refs[:-1], refs[-1]
    for dz, block in zip(shifts, blocks):
        merge(takes_ref, own_ref, block, merged, [unit_at(line, dz, -1) for line in range(LINES)])


def unpack_late_kernel(shifts, takes_ref, own_ref, early_ref, block, *refs):
    out_ref, merged, sem = refs

    def place(line, carry):
        unit = unit_at(line, shifts[0], -1)
        for r in range(LIMIT):
            start = takes_ref[r, unit]
            own = own_ref[row_at(jnp.where(start < FLAT, start, 0)), :]
            merged[row_at(start), :] = (own + block[cell(line, r), :]) * 0.5
        return carry

    lax.fori_loop(0, LINES, place, 0)
    store(merged, out_ref, sem)


def tiles_of(x):
    return x.reshape(ROWS // 8, 8, TALL, 128).transpose(0, 2, 1, 3).reshape(FLAT, 128)


def rows_of(x):
    return x.reshape(ROWS // 8, TALL, 8, 128).transpose(0, 2, 1, 3).reshape(ROWS, WIDTH)


def sent(block, dx, dz, dc):
    def at(x, z, c):
        return (x % NX * NZ + z % NZ) * NC + c % NC

    pairs = [
        (at(x, z, c), at(x + dx, z + dz, c + dc)) for x in range(NX) for z in range(NZ) for c in range(NC)
    ]
    return lax.ppermute(block, UNITS, pairs)


def in_order(blocks, order):
    return [blocks[-1]] + [blocks[order.index(i)] for i in range(1, 8)]


def by_z(blocks, order):
    blocks = list(blocks)
    for dz in order:
        blocks[dz] = sent(blocks[dz], 0, dz, 0)
    return blocks


def by_line(blocks):
    blocks = list(blocks)
    for line in LINE_ORDER:
        blocks[line] = sent(blocks[line], line >> 1, 0, line & 1)
    return blocks


VMEM = pl.BlockSpec(memory_space=pltpu.VMEM)
SMEM = pl.BlockSpec(memory_space=pltpu.SMEM)
HBM = pl.BlockSpec(memory_space=pltpu.HBM)
PACKED = (jax.ShapeDtypeStruct((BLOCK, 128), jnp.float32),) * 8
MERGED = (FLAT + 8 * TALL, 128)
SEMS = pltpu.SemaphoreType.DMA((STORES,))
SCRATCH = [pltpu.VMEM(MERGED, jnp.float32), SEMS]


def call(kernel, out, specs, out_specs, scratch=(), flops=500_000_000, aliases=None):
    return pl.pallas_call(
        kernel,
        out_shape=out,
        in_specs=specs,
        out_specs=out_specs,
        scratch_shapes=list(scratch),
        input_output_aliases=aliases or {},
        cost_estimate=pl.CostEstimate(flops=flops, bytes_accessed=1 << 20, transcendentals=0),
        compiler_params=pltpu.CompilerParams(vmem_limit_bytes=12 << 20),
    )


def on_device(a_up, a_down, b_up, b_down, perm):
    out = jax.ShapeDtypeStruct((FLAT, 128), jnp.float32)
    table = jax.ShapeDtypeStruct((8, 128), jnp.int32)
    perm = perm.reshape(COUNT * ROWS // 128, 128)
    sends, takes = call(tables_kernel, (table, table), [VMEM, VMEM], (VMEM, VMEM), flops=700_000_000)(
        (perm >> 7).astype(jnp.float32), (perm & 127).astype(jnp.float32)
    )
    down = []
    for shifts in (Z_ORDER[:1], Z_ORDER[1:] + (0,)):
        down += call(
            functools.partial(pack_by_z_kernel, shifts), PACKED[: len(shifts)], [SMEM, VMEM], (VMEM,) * len(shifts)
        )(sends, tiles_of(b_down))
    down = by_z(in_order(down, Z_ORDER), Z_ORDER)
    up = call(pack_by_line_kernel, PACKED, [SMEM, VMEM], (VMEM,) * 8)(sends, tiles_of(b_up))
    up = by_line(in_order(up, LINE_ORDER))
    up = call(turn_kernel, PACKED, [VMEM] * 8, (VMEM,) * 8)(*up)
    up = by_z(up, Z_LAST)
    down = call(turn_kernel, PACKED, [VMEM] * 8, (VMEM,) * 8)(*down)
    down = by_line(down)
    merged_down = call(
        unpack_by_line_kernel, out, [SMEM, VMEM] + [VMEM] * LINES, HBM, SCRATCH
    )(takes, tiles_of(a_down), *down)
    late = Z_LAST[-1:]
    early = (0,) + Z_LAST[:-1]
    own = tiles_of(a_up)
    merged_up = call(
        functools.partial(unpack_early_kernel, early),
        jax.ShapeDtypeStruct(MERGED, jnp.float32),
        [SMEM, VMEM] + [VMEM] * len(early),
        VMEM,
    )(takes, own, *[up[dz] for dz in early])
    merged_up, _ = call(
        functools.partial(unpack_late_kernel, late),
        (out, jax.ShapeDtypeStruct(MERGED, jnp.float32)),
        [SMEM, VMEM, VMEM] + [VMEM] * len(late),
        (HBM, VMEM),
        [SEMS],
        aliases={2: 1},
    )(takes, own, merged_up, *[up[dz] for dz in late])
    return rows_of(merged_up), rows_of(merged_down)


def solution(mesh):
    finer = Mesh(
        mesh.devices.reshape(NX, NZ, NC, mesh.shape["expert"]),
        ("units_0", "units_1", "units_2", "expert"),
    )
    rows = P(EXPERT_UNITS, None)
    return jax.shard_map(
        on_device,
        mesh=finer,
        in_specs=(rows, rows, rows, rows, P("expert")),
        out_specs=(rows, rows),
        check_vma=False,
    )
```
